8 devices in a mesh: rep: 2 (over z, y), blk: 4 (over x, core).
Axes of the slice: x: 2, y: 2, z: 1, core: 2. Of those that a mesh axis runs over, the one named last changes fastest.
Arguments:
- ratings: float32 [4096, 16384], P(None, ('rep', 'blk')), parts along dimension 1
- observed: int32 [4096, 16384], P(None, ('rep', 'blk')), parts along dimension 1
- user_init: float32 [8192, 256], P(('rep', 'blk')), parts along dimension 0
- item_init: float32 [16384, 256], P(('rep', 'blk')), parts along dimension 0
- lr_scale: float32 [64, 1], replicated
Outputs:
- output 1: float32 [8192, 256], P(('rep', 'blk')), parts along dimension 0
- output 2: float32 [16384, 256], P(('rep', 'blk')), parts along dimension 0
There are 2 independent parts. The reference program is written for one: setup_inputs(seed, part) draws one part's arguments, and reference() takes and returns one part's arrays. A program takes and returns all parts, laid end to end along the dimension named above; an argument that names none is the same for every part.
All inputs are finite; a program needn't handle non-finite values.
Results may differ from the reference program's by a relative error of at most 0.001.
Values are sent between devices in bfloat16 or wider.
A program may use at most 1 GiB of HBM per device.

```python
import math
import jax
import jax.numpy as jnp
from jax import lax

USERS = 4096
COLS_DEV = 2048
RANK = 256
NUM_BLOCKS = 4
STEPS = 1
EPOCHS = 16
NUM_ITEMS = NUM_BLOCKS * COLS_DEV
BLOCK_ROWS = USERS // NUM_BLOCKS
STEP_BASE = math.sqrt(RANK) / (4.0 * (COLS_DEV + 2 * RANK))
LAMBDA = 0.05
INIT_SCALE = RANK ** -0.25


def setup_inputs(seed: int = 0, part: int = 0) -> dict:
    base_key = jax.random.key(seed)
    shared_key, part_root = jax.random.split(base_key)
    part_key = jax.random.fold_in(part_root, part)
    key_list = jax.random.split(part_key, 7)
    left_true = jax.random.normal(key_list[0], (USERS, RANK), jnp.float32) * INIT_SCALE
    right_true = jax.random.normal(key_list[1], (NUM_ITEMS, RANK), jnp.float32) * INIT_SCALE
    noise_draw = jax.random.normal(key_list[2], (USERS, NUM_ITEMS), jnp.float32)
    ratings = jnp.dot(left_true, right_true.T) + 0.3 * noise_draw
    row_pct = jax.random.randint(key_list[3], (USERS, 1), 10, 41)
    pct_draws = jax.random.randint(key_list[4], (USERS, NUM_ITEMS), 0, 100)
    observed = (pct_draws < row_pct).astype(jnp.int32)
    user_init = jax.random.normal(key_list[5], (USERS, RANK), jnp.float32) * INIT_SCALE
    item_init = jax.random.normal(key_list[6], (NUM_ITEMS, RANK), jnp.float32) * INIT_SCALE
    lr_scale = jax.random.uniform(shared_key, (EPOCHS * NUM_BLOCKS, STEPS), jnp.float32, 0.25, 1.0)
    return {"ratings": ratings, "observed": observed, "user_init": user_init, "item_init": item_init, "lr_scale": lr_scale}


def as_bf16_values(values):
    return values.astype(jnp.bfloat16).astype(jnp.float32)


def reference(ratings, observed, user_init, item_init, lr_scale):
    rate_grid = ratings.reshape(NUM_BLOCKS, BLOCK_ROWS, NUM_BLOCKS, COLS_DEV)
    mask_grid = observed.astype(jnp.float32).reshape(NUM_BLOCKS, BLOCK_ROWS, NUM_BLOCKS, COLS_DEV)
    item_ids = jnp.arange(NUM_BLOCKS)

    def sub_epoch(carry, step_inputs):
        user_blocks, item_blocks = carry
        t_index, scales = step_inputs
        user_ids = (item_ids + t_index) % NUM_BLOCKS
        rate_now = rate_grid[user_ids, :, item_ids, :]
        mask_now = mask_grid[user_ids, :, item_ids, :]

        def one_step(step_state, scale_val):
            users_cur, items_cur = step_state
            users_bf = as_bf16_values(users_cur)
            items_bf = as_bf16_values(items_cur)
            approx = jnp.einsum("jar,jbr->jab", users_bf, items_bf)
            errors = as_bf16_values(mask_now * (approx - rate_now))
            grad_u = jnp.einsum("jab,jbr->jar", errors, items_bf) + LAMBDA * users_cur
            grad_v = jnp.einsum("jab,jar->jbr", errors, users_bf) + LAMBDA * items_cur
            step_size = STEP_BASE * scale_val
            return (users_cur - step_size * grad_u, items_cur - step_size * grad_v), None

        (users_new, items_new), _ = lax.scan(one_step, (user_blocks[user_ids], item_blocks), scales)
        home_ids = (item_ids - t_index) % NUM_BLOCKS
        return (users_new[home_ids], items_new), None

    user_blocks = user_init.reshape(NUM_BLOCKS, BLOCK_ROWS, RANK)
    item_blocks = item_init.reshape(NUM_BLOCKS, COLS_DEV, RANK)
    t_values = jnp.arange(EPOCHS * NUM_BLOCKS) % NUM_BLOCKS
    (user_blocks, item_blocks), _ = lax.scan(sub_epoch, (user_blocks, item_blocks), (t_values, lr_scale))
    return user_blocks.reshape(USERS, RANK), item_blocks.reshape(NUM_ITEMS, RANK)
```

```python
import functools
import math

import jax
import jax.numpy as jnp
from jax import lax
from jax.experimental import pallas as pl
from jax.experimental.pallas import tpu as pltpu
from jax.sharding import PartitionSpec as P

LAMBDA = 0.05
MESH = pl.DeviceIdType.MESH
CHUNK = 256
TILE = 512
STAGES = 3


def run_kernel(group, epochs_t, base_eta, lr_ref, r_hbm, m_hbm, u_hbm, v_hbm, uo_hbm, vo_hbm,
               rate, mask, v, vb, gv, err, inb, outb, load_sem, r_sem, m_sem, send_sem, recv_sem, home_sem, credit):
    rep, me = lax.axis_index("rep"), lax.axis_index("blk")
    left, right = lax.rem(me + group - 1, group), lax.rem(me + 1, group)
    chunks = inb.shape[1]
    items = v.shape[0]
    loads = group * chunks

    def row_block(g):
        return lax.rem(me + g // chunks, group) * chunks + lax.rem(g, chunks)

    def rate_load(g):
        where = row_block(g)
        return pltpu.make_async_copy(r_hbm.at[pl.ds(pl.multiple_of(where * CHUNK, CHUNK), CHUNK)], rate.at[where], r_sem.at[lax.rem(g, STAGES)])

    def mask_load(g):
        where = row_block(g)
        slot = lax.rem(g, STAGES)
        return pltpu.make_async_copy(m_hbm.at[pl.ds(pl.multiple_of(where * CHUNK, CHUNK), CHUNK)], mask.at[slot], m_sem.at[slot])

    def send(t, c):
        slot = lax.rem(t, 2)
        return pltpu.make_async_remote_copy(
            src_ref=outb.at[slot, c], dst_ref=inb.at[1 - slot, c], send_sem=send_sem.at[slot, c],
            recv_sem=recv_sem.at[1 - slot, c], device_id=(rep, left), device_id_type=MESH)

    def send_home(t, c):
        slot = lax.rem(t, 2)
        return pltpu.make_async_remote_copy(
            src_ref=outb.at[slot, c], dst_ref=uo_hbm.at[pl.ds(pl.multiple_of(c * CHUNK, CHUNK), CHUNK)], send_sem=send_sem.at[slot, c],
            recv_sem=home_sem.at[c], device_id=(rep, left), device_id_type=MESH)

    def user_load(c):
        return pltpu.make_async_copy(u_hbm.at[pl.ds(c * CHUNK, CHUNK)], inb.at[0, c], recv_sem.at[0, c])

    v_load = pltpu.make_async_copy(v_hbm, v, load_sem)
    v_load.start()
    user_load(0).start()
    rate_load(0).start()
    mask_load(0).start()
    for c in range(1, chunks):
        user_load(c).start()
    rate_load(1).start()
    mask_load(1).start()

    barrier = pltpu.get_barrier_semaphore()
    for neighbour in (left, right):
        pl.semaphore_signal(barrier, inc=1, device_id=(rep, neighbour), device_id_type=MESH)
    pl.semaphore_wait(barrier, 2)

    gv[...] = jnp.zeros_like(gv)
    v_load.wait()
    vb[...] = v[...].astype(jnp.bfloat16)

    def chunk_step(t, c, step_size, first):
        slot = lax.rem(t, 2)
        if first:
            g = t * chunks + c

            @pl.when(g + 2 < loads)
            def _():
                rate_load(g + 2).start()
                mask_load(g + 2).start()

            rate_load(g).wait()
            mask_load(g).wait()

        @pl.when(t == 0)
        def _():
            pltpu.make_async_copy(u_hbm.at[pl.ds(0, CHUNK)], inb.at[0, c], recv_sem.at[0, c]).wait()

        @pl.when(t > 0)
        def _():
            send(t - 1, c).wait_recv()

        @pl.when(t >= 2)
        def _():
            send(t, c).wait_send()

        where = lax.rem(me + t, group) * chunks + c
        users_bf = inb[slot, c].astype(jnp.bfloat16)
        for n in range(items // TILE):
            cols = pl.ds(n * TILE, TILE)
            approx = lax.dot_general(users_bf, vb[cols, :], (((1,), (1,)), ((), ())), preferred_element_type=jnp.float32)
            rates = rate[where, :, cols]
            if first:
                seen = mask[lax.rem(t * chunks + c, STAGES), :, cols] != 0
                rate[where, :, cols] = jnp.where(seen, rates, jnp.inf)
            else:
                seen = rates < jnp.inf
            err[:, cols] = jnp.where(seen, approx - rates, 0.0).astype(jnp.bfloat16)
        grad_u = jnp.dot(err[...], vb[...], preferred_element_type=jnp.float32)
        users = inb[slot, c]
        outb[slot, c] = users - step_size * (grad_u + LAMBDA * users)

        for n in range(items // TILE):
            cols = pl.ds(n * TILE, TILE)
            gv[cols, :] += lax.dot_general(err[:, cols], users_bf, (((0,), (0,)), ((), ())), preferred_element_type=jnp.float32)

        @pl.when(t < epochs_t - 2)
        def _():
            pl.semaphore_signal(credit, inc=1, device_id=(rep, right), device_id_type=MESH)

        @pl.when((t > 0) & (t < epochs_t - 1))
        def _():
            pl.semaphore_wait(credit, 1)

        @pl.when(t < epochs_t - 1)
        def _():
            send(t, c).start()

        @pl.when(t == epochs_t - 1)
        def _():
            send_home(t, c).start()

    def sub_epoch(first, t, carry):
        step_size = base_eta * lr_ref[t, 0]

        def body(c, inner):
            chunk_step(t, c, step_size, first)
            return inner

        lax.fori_loop(0, chunks, body, 0)
        for n in range(items // TILE):
            cols = pl.ds(n * TILE, TILE)
            old = v[cols, :]
            new = old - step_size * (gv[cols, :] + LAMBDA * old)
            v[cols, :] = new
            vb[cols, :] = new.astype(jnp.bfloat16)
            gv[cols, :] = jnp.zeros((TILE, v.shape[1]), jnp.float32)
        return carry

    lax.fori_loop(0, group, functools.partial(sub_epoch, True), 0)
    lax.fori_loop(group, epochs_t, functools.partial(sub_epoch, False), 0)

    v_store = pltpu.make_async_copy(v, vo_hbm, load_sem)
    v_store.start()
    v_store.wait()
    for c in range(chunks):
        send(epochs_t - 2, c).wait_send()
        send_home(epochs_t - 1, c).wait_send()
        send_home(epochs_t - 1, c).wait_recv()


def solution(mesh):
    group = mesh.shape["blk"]

    def local_run(rate_loc, mask_loc, user_loc, item_loc, lr_scale):
        block_rows, rank = user_loc.shape
        items = item_loc.shape[0]
        epochs_t = lr_scale.shape[0]
        chunks = block_rows // CHUNK
        base_eta = math.sqrt(rank) / (4.0 * (items + 2 * rank))
        hbm = pl.BlockSpec(memory_space=pl.ANY)
        return pl.pallas_call(
            functools.partial(run_kernel, group, epochs_t, base_eta),
            out_shape=(jax.ShapeDtypeStruct(user_loc.shape, jnp.float32), jax.ShapeDtypeStruct(item_loc.shape, jnp.float32)),
            in_specs=[pl.BlockSpec(memory_space=pltpu.SMEM), hbm, hbm, hbm, hbm],
            out_specs=(hbm, hbm),
            scratch_shapes=[
                pltpu.VMEM((group * chunks, CHUNK, items), jnp.float32),
                pltpu.VMEM((STAGES, CHUNK, items), jnp.int32),
                pltpu.VMEM((items, rank), jnp.float32),
                pltpu.VMEM((items, rank), jnp.bfloat16),
                pltpu.VMEM((items, rank), jnp.float32),
                pltpu.VMEM((CHUNK, items), jnp.bfloat16),
                pltpu.VMEM((2, chunks, CHUNK, rank), jnp.float32),
                pltpu.VMEM((2, chunks, CHUNK, rank), jnp.float32),
                pltpu.SemaphoreType.DMA,
                pltpu.SemaphoreType.DMA((STAGES,)),
                pltpu.SemaphoreType.DMA((STAGES,)),
                pltpu.SemaphoreType.DMA((2, chunks)),
                pltpu.SemaphoreType.DMA((2, chunks)),
                pltpu.SemaphoreType.DMA((chunks,)),
                pltpu.SemaphoreType.REGULAR,
            ],
            compiler_params=pltpu.CompilerParams(collective_id=0, has_side_effects=True, vmem_limit_bytes=67_043_328),
        )(lr_scale, rate_loc, mask_loc, user_loc, item_loc)

    spec_cols = P(None, ("rep", "blk"))
    spec_rows = P(("rep", "blk"), None)
    return jax.shard_map(local_run, mesh=mesh, in_specs=(spec_cols, spec_cols, spec_rows, spec_rows, P(None, None)),
                         out_specs=(spec_rows, spec_rows), check_vma=False)
```

```python
import functools
import math

import jax
import jax.numpy as jnp
from jax import lax
from jax.experimental import pallas as pl
from jax.experimental.pallas import tpu as pltpu
from jax.sharding import PartitionSpec as P

LAMBDA = 0.05
MESH = pl.DeviceIdType.MESH
CHUNK = 128
TILE = 512
STAGES = 3


def run_kernel(group, epochs_t, base_eta, lr_hbm, r_hbm, m_hbm, u_hbm, v_hbm, uo_hbm, vo_hbm,
               lr, rate, mask, v, vb, gv, err, inb, outb, load_sem, r_sem, m_sem, send_sem, recv_sem, home_sem, lr_sem, credit):
    rep, me = lax.axis_index("rep"), lax.axis_index("blk")
    left, right = lax.rem(me + group - 1, group), lax.rem(me + 1, group)
    chunks = inb.shape[1]
    items = v.shape[0]
    loads = group * chunks

    def row_block(g):
        return lax.rem(me + g // chunks, group) * chunks + lax.rem(g, chunks)

    def rate_load(g):
        where = row_block(g)
        return pltpu.make_async_copy(r_hbm.at[pl.ds(pl.multiple_of(where * CHUNK, CHUNK), CHUNK)], rate.at[where], r_sem.at[lax.rem(g, STAGES)])

    def mask_load(g):
        where = row_block(g)
        slot = lax.rem(g, STAGES)
        return pltpu.make_async_copy(m_hbm.at[pl.ds(pl.multiple_of(where * CHUNK, CHUNK), CHUNK)], mask.at[slot], m_sem.at[slot])

    def send(t, c):
        slot = lax.rem(t, 2)
        return pltpu.make_async_remote_copy(
            src_ref=outb.at[slot, c], dst_ref=inb.at[1 - slot, c], send_sem=send_sem.at[slot, c],
            recv_sem=recv_sem.at[1 - slot, c], device_id=(rep, left), device_id_type=MESH)

    def send_home(t, c):
        slot = lax.rem(t, 2)
        return pltpu.make_async_remote_copy(
            src_ref=outb.at[slot, c], dst_ref=uo_hbm.at[pl.ds(pl.multiple_of(c * CHUNK, CHUNK), CHUNK)], send_sem=send_sem.at[slot, c],
            recv_sem=home_sem.at[c], device_id=(rep, left), device_id_type=MESH)

    def user_load(c):
        return pltpu.make_async_copy(u_hbm.at[pl.ds(c * CHUNK, CHUNK)], inb.at[0, c], recv_sem.at[0, c])

    def v_load(n):
        cols = pl.ds(n * TILE, TILE)
        return pltpu.make_async_copy(v_hbm.at[cols], v.at[cols], load_sem.at[n])

    tiles = items // TILE
    for n in range(tiles):
        v_load(n).start()
    user_load(0).start()
    rate_load(0).start()
    mask_load(0).start()
    lr_load = pltpu.make_async_copy(lr_hbm, lr, lr_sem)
    lr_load.start()
    for c in range(1, chunks):
        user_load(c).start()

    barrier = pltpu.get_barrier_semaphore()
    for neighbour in (left, right):
        pl.semaphore_signal(barrier, inc=1, device_id=(rep, neighbour), device_id_type=MESH)
    gv[...] = jnp.zeros_like(gv)
    for n in range(tiles):
        cols = pl.ds(n * TILE, TILE)
        v_load(n).wait()
        vb[cols, :] = v[cols, :].astype(jnp.bfloat16)
    lr_load.wait()
    pl.semaphore_wait(barrier, 2)
    rate_load(1).start()
    mask_load(1).start()

    def chunk_step(t, c, step_size, first):
        slot = lax.rem(t, 2)
        if first:
            g = t * chunks + c

            @pl.when(g + 2 < loads)
            def _():
                rate_load(g + 2).start()
                mask_load(g + 2).start()

            rate_load(g).wait()
            mask_load(g).wait()

        @pl.when(t == 0)
        def _():
            pltpu.make_async_copy(u_hbm.at[pl.ds(0, CHUNK)], inb.at[0, c], recv_sem.at[0, c]).wait()

        @pl.when(t > 0)
        def _():
            send(t - 1, c).wait_recv()

        @pl.when(t >= 2)
        def _():
            send(t, c).wait_send()

        where = lax.rem(me + t, group) * chunks + c
        users_bf = inb[slot, c].astype(jnp.bfloat16)
        for n in range(items // TILE):
            cols = pl.ds(n * TILE, TILE)
            approx = lax.dot_general(users_bf, vb[cols, :], (((1,), (1,)), ((), ())), preferred_element_type=jnp.float32)
            rates = rate[where, :, cols]
            if first:
                seen = mask[lax.rem(t * chunks + c, STAGES), :, cols] != 0
                rate[where, :, cols] = jnp.where(seen, rates, jnp.inf)
            else:
                seen = rates < jnp.inf
            err[:, cols] = jnp.where(seen, approx - rates, 0.0).astype(jnp.bfloat16)
        grad_u = jnp.dot(err[...], vb[...], preferred_element_type=jnp.float32)
        users = inb[slot, c]
        outb[slot, c] = users - step_size * (grad_u + LAMBDA * users)

        for n in range(items // TILE):
            cols = pl.ds(n * TILE, TILE)
            gv[cols, :] += lax.dot_general(err[:, cols], users_bf, (((0,), (0,)), ((), ())), preferred_element_type=jnp.float32)

        @pl.when(t < epochs_t - 2)
        def _():
            pl.semaphore_signal(credit, inc=1, device_id=(rep, right), device_id_type=MESH)

        @pl.when((t > 0) & (t < epochs_t - 1))
        def _():
            pl.semaphore_wait(credit, 1)

        @pl.when(t < epochs_t - 1)
        def _():
            send(t, c).start()

        @pl.when(t == epochs_t - 1)
        def _():
            send_home(t, c).start()

    def sub_epoch(first, t, carry):
        step_size = base_eta * lr[t]

        def body(c, inner):
            chunk_step(t, c, step_size, first)
            return inner

        lax.fori_loop(0, chunks, body, 0)
        for n in range(items // TILE):
            cols = pl.ds(n * TILE, TILE)
            old = v[cols, :]
            new = old - step_size * (gv[cols, :] + LAMBDA * old)
            v[cols, :] = new
            vb[cols, :] = new.astype(jnp.bfloat16)
            gv[cols, :] = jnp.zeros((TILE, v.shape[1]), jnp.float32)
        return carry

    lax.fori_loop(0, group, functools.partial(sub_epoch, True), 0)
    lax.fori_loop(group, epochs_t, functools.partial(sub_epoch, False), 0)

    vo_hbm[...] = v[...]
    for c in range(chunks):
        send(epochs_t - 2, c).wait_send()
        send_home(epochs_t - 1, c).wait_send()
        send_home(epochs_t - 1, c).wait_recv()


PARTS = 4


def write_out(u_vmem, v_vmem, uo_hbm, vo_hbm, sem):
    copies = []
    for k, (src, dst) in enumerate(((v_vmem, vo_hbm), (u_vmem, uo_hbm))):
        rows = src.shape[0] // PARTS
        for p in range(PARTS):
            part = pl.ds(p * rows, rows)
            copies.append(pltpu.make_async_copy(src.at[part], dst.at[part], sem.at[k, p]))
    for copy in copies:
        copy.start()
    for copy in copies:
        copy.wait()


def solution(mesh):
    group = mesh.shape["blk"]

    def local_run(rate_loc, mask_loc, user_loc, item_loc, lr_scale):
        block_rows, rank = user_loc.shape
        cols = item_loc.shape[0]
        epochs_t = lr_scale.shape[0]
        chunks = block_rows // CHUNK
        base_eta = math.sqrt(rank) / (4.0 * (cols + 2 * rank))
        vmem = pl.BlockSpec(memory_space=pltpu.VMEM)
        hbm = pl.BlockSpec(memory_space=pl.ANY)
        users, items = pl.pallas_call(
            functools.partial(run_kernel, group, epochs_t, base_eta),
            out_shape=(pltpu.VMEM(user_loc.shape, jnp.float32), pltpu.VMEM(item_loc.shape, jnp.float32)),
            in_specs=[hbm, hbm, hbm, hbm, hbm],
            out_specs=(vmem, vmem),
            scratch_shapes=[
                pltpu.SMEM((epochs_t,), jnp.float32),
                pltpu.VMEM((group * chunks, CHUNK, cols), jnp.float32),
                pltpu.VMEM((STAGES, CHUNK, cols), jnp.int32),
                pltpu.VMEM((cols, rank), jnp.float32),
                pltpu.VMEM((cols, rank), jnp.bfloat16),
                pltpu.VMEM((cols, rank), jnp.float32),
                pltpu.VMEM((CHUNK, cols), jnp.bfloat16),
                pltpu.VMEM((2, chunks, CHUNK, rank), jnp.float32),
                pltpu.VMEM((2, chunks, CHUNK, rank), jnp.float32),
                pltpu.SemaphoreType.DMA((cols // TILE,)),
                pltpu.SemaphoreType.DMA((STAGES,)),
                pltpu.SemaphoreType.DMA((STAGES,)),
                pltpu.SemaphoreType.DMA((2, chunks)),
                pltpu.SemaphoreType.DMA((2, chunks)),
                pltpu.SemaphoreType.DMA((chunks,)),
                pltpu.SemaphoreType.DMA,
                pltpu.SemaphoreType.REGULAR,
            ],
            compiler_params=pltpu.CompilerParams(collective_id=0, has_side_effects=True, vmem_limit_bytes=56*1024*1024),
        )(lr_scale.reshape(epochs_t), rate_loc, mask_loc, user_loc, item_loc)
        return pl.pallas_call(
            write_out,
            out_shape=(jax.ShapeDtypeStruct(user_loc.shape, jnp.float32), jax.ShapeDtypeStruct(item_loc.shape, jnp.float32)),
            in_specs=[vmem, vmem],
            out_specs=(hbm, hbm),
            scratch_shapes=[pltpu.SemaphoreType.DMA((2, PARTS))],
            compiler_params=pltpu.CompilerParams(vmem_limit_bytes=1024 * 1024),
        )(users, items)

    spec_cols = P(None, ("rep", "blk"))
    spec_rows = P(("rep", "blk"), None)
    return jax.shard_map(local_run, mesh=mesh, in_specs=(spec_cols, spec_cols, spec_rows, spec_rows, P(None, None)),
                         out_specs=(spec_rows, spec_rows), check_vma=False)
```

```python
import functools
import math

import jax
import jax.numpy as jnp
from jax import lax
from jax.experimental import pallas as pl
from jax.experimental.pallas import tpu as pltpu
from jax.sharding import PartitionSpec as P

LAMBDA = 0.05
MESH = pl.DeviceIdType.MESH
CHUNK = 128
TILE = 512
STAGES = 3


def run_kernel(group, epochs_t, base_eta, lr_hbm, r_hbm, m_hbm, u_hbm, v_hbm, uo_hbm, vo_hbm,
               lr, rate, mask, v, vb, gv, err, inb, outb, load_sem, r_sem, m_sem, send_sem, recv_sem, home_sem, lr_sem, credit):
    rep, me = lax.axis_index("rep"), lax.axis_index("blk")
    left, right = lax.rem(me + group - 1, group), lax.rem(me + 1, group)
    chunks = inb.shape[1]
    items = v.shape[0]
    loads = group * chunks

    def row_block(g):
        return lax.rem(me + g // chunks, group) * chunks + lax.rem(g, chunks)

    def rate_load(g):
        where = row_block(g)
        return pltpu.make_async_copy(r_hbm.at[pl.ds(pl.multiple_of(where * CHUNK, CHUNK), CHUNK)], rate.at[where], r_sem.at[lax.rem(g, STAGES)])

    def mask_load(g):
        where = row_block(g)
        slot = lax.rem(g, STAGES)
        return pltpu.make_async_copy(m_hbm.at[pl.ds(pl.multiple_of(where * CHUNK, CHUNK), CHUNK)], mask.at[slot], m_sem.at[slot])

    def send(t, c):
        slot = lax.rem(t, 2)
        return pltpu.make_async_remote_copy(
            src_ref=outb.at[slot, c], dst_ref=inb.at[1 - slot, c], send_sem=send_sem.at[slot, c],
            recv_sem=recv_sem.at[1 - slot, c], device_id=(rep, left), device_id_type=MESH)

    def send_home(t, c):
        slot = lax.rem(t, 2)
        return pltpu.make_async_remote_copy(
            src_ref=outb.at[slot, c], dst_ref=uo_hbm.at[pl.ds(pl.multiple_of(c * CHUNK, CHUNK), CHUNK)], send_sem=send_sem.at[slot, c],
            recv_sem=home_sem.at[c], device_id=(rep, left), device_id_type=MESH)

    def user_load(c):
        return pltpu.make_async_copy(u_hbm.at[pl.ds(c * CHUNK, CHUNK)], inb.at[0, c], recv_sem.at[0, c])

    def v_load(n):
        cols = pl.ds(n * TILE, TILE)
        return pltpu.make_async_copy(v_hbm.at[cols], v.at[cols], load_sem.at[n])

    tiles = items // TILE
    for n in range(tiles):
        v_load(n).start()
    user_load(0).start()
    rate_load(0).start()
    mask_load(0).start()
    lr_load = pltpu.make_async_copy(lr_hbm, lr, lr_sem)
    lr_load.start()

    barrier = pltpu.get_barrier_semaphore()
    for neighbour in (left, right):
        pl.semaphore_signal(barrier, inc=1, device_id=(rep, neighbour), device_id_type=MESH)
    gv[...] = jnp.zeros_like(gv)
    for n in range(tiles):
        cols = pl.ds(n * TILE, TILE)
        v_load(n).wait()
        vb[cols, :] = v[cols, :].astype(jnp.bfloat16)
    lr_load.wait()
    pl.semaphore_wait(barrier, 2)
    rate_load(1).start()
    mask_load(1).start()
    for c in range(1, chunks):
        user_load(c).start()

    def chunk_step(t, c, step_size, first):
        slot = lax.rem(t, 2)
        if first:
            g = t * chunks + c

            @pl.when(g + 2 < loads)
            def _():
                rate_load(g + 2).start()
                mask_load(g + 2).start()

            rate_load(g).wait()
            mask_load(g).wait()

        @pl.when(t == 0)
        def _():
            pltpu.make_async_copy(u_hbm.at[pl.ds(0, CHUNK)], inb.at[0, c], recv_sem.at[0, c]).wait()

        @pl.when(t > 0)
        def _():
            send(t - 1, c).wait_recv()

        @pl.when(t >= 2)
        def _():
            send(t, c).wait_send()

        where = lax.rem(me + t, group) * chunks + c
        users_bf = inb[slot, c].astype(jnp.bfloat16)
        for n in range(items // TILE):
            cols = pl.ds(n * TILE, TILE)
            approx = lax.dot_general(users_bf, vb[cols, :], (((1,), (1,)), ((), ())), preferred_element_type=jnp.float32)
            rates = rate[where, :, cols]
            if first:
                seen = mask[lax.rem(t * chunks + c, STAGES), :, cols] != 0
                rate[where, :, cols] = jnp.where(seen, rates, jnp.inf)
            else:
                seen = rates < jnp.inf
            err[:, cols] = jnp.where(seen, approx - rates, 0.0).astype(jnp.bfloat16)
        grad_u = jnp.dot(err[...], vb[...], preferred_element_type=jnp.float32)
        users = inb[slot, c]
        outb[slot, c] = users - step_size * (grad_u + LAMBDA * users)

        for n in range(items // TILE):
            cols = pl.ds(n * TILE, TILE)
            gv[cols, :] += lax.dot_general(err[:, cols], users_bf, (((0,), (0,)), ((), ())), preferred_element_type=jnp.float32)

        @pl.when(t < epochs_t - 2)
        def _():
            pl.semaphore_signal(credit, inc=1, device_id=(rep, right), device_id_type=MESH)

        @pl.when((t > 0) & (t < epochs_t - 1))
        def _():
            pl.semaphore_wait(credit, 1)

        @pl.when(t < epochs_t - 1)
        def _():
            send(t, c).start()

        @pl.when(t == epochs_t - 1)
        def _():
            send_home(t, c).start()

    def sub_epoch(first, t, carry):
        step_size = base_eta * lr[t]

        def body(c, inner):
            chunk_step(t, c, step_size, first)
            return inner

        lax.fori_loop(0, chunks, body, 0)
        for n in range(items // TILE):
            cols = pl.ds(n * TILE, TILE)
            old = v[cols, :]
            new = old - step_size * (gv[cols, :] + LAMBDA * old)
            v[cols, :] = new
            vb[cols, :] = new.astype(jnp.bfloat16)
            gv[cols, :] = jnp.zeros((TILE, v.shape[1]), jnp.float32)
        return carry

    lax.fori_loop(0, group, functools.partial(sub_epoch, True), 0)
    lax.fori_loop(group, epochs_t, functools.partial(sub_epoch, False), 0)

    vo_hbm[...] = v[...]
    for c in range(chunks):
        send(epochs_t - 2, c).wait_send()
        send_home(epochs_t - 1, c).wait_send()
        send_home(epochs_t - 1, c).wait_recv()


PARTS = 2


def write_out(u_vmem, v_vmem, uo_hbm, vo_hbm, sem):
    copies = []
    for k, (src, dst) in enumerate(((v_vmem, vo_hbm), (u_vmem, uo_hbm))):
        rows = src.shape[0] // PARTS
        for p in range(PARTS):
            part = pl.ds(p * rows, rows)
            copies.append(pltpu.make_async_copy(src.at[part], dst.at[part], sem.at[k, p]))
    for copy in copies:
        copy.start()
    for copy in copies:
        copy.wait()


def solution(mesh):
    group = mesh.shape["blk"]

    def local_run(rate_loc, mask_loc, user_loc, item_loc, lr_scale):
        block_rows, rank = user_loc.shape
        cols = item_loc.shape[0]
        epochs_t = lr_scale.shape[0]
        chunks = block_rows // CHUNK
        base_eta = math.sqrt(rank) / (4.0 * (cols + 2 * rank))
        vmem = pl.BlockSpec(memory_space=pltpu.VMEM)
        hbm = pl.BlockSpec(memory_space=pl.ANY)
        users, items = pl.pallas_call(
            functools.partial(run_kernel, group, epochs_t, base_eta),
            out_shape=(pltpu.VMEM(user_loc.shape, jnp.float32), pltpu.VMEM(item_loc.shape, jnp.float32)),
            in_specs=[hbm, hbm, hbm, hbm, hbm],
            out_specs=(vmem, vmem),
            scratch_shapes=[
                pltpu.SMEM((epochs_t,), jnp.float32),
                pltpu.VMEM((group * chunks, CHUNK, cols), jnp.float32),
                pltpu.VMEM((STAGES, CHUNK, cols), jnp.int32),
                pltpu.VMEM((cols, rank), jnp.float32),
                pltpu.VMEM((cols, rank), jnp.bfloat16),
                pltpu.VMEM((cols, rank), jnp.float32),
                pltpu.VMEM((CHUNK, cols), jnp.bfloat16),
                pltpu.VMEM((2, chunks, CHUNK, rank), jnp.float32),
                pltpu.VMEM((2, chunks, CHUNK, rank), jnp.float32),
                pltpu.SemaphoreType.DMA((cols // TILE,)),
                pltpu.SemaphoreType.DMA((STAGES,)),
                pltpu.SemaphoreType.DMA((STAGES,)),
                pltpu.SemaphoreType.DMA((2, chunks)),
                pltpu.SemaphoreType.DMA((2, chunks)),
                pltpu.SemaphoreType.DMA((chunks,)),
                pltpu.SemaphoreType.DMA,
                pltpu.SemaphoreType.REGULAR,
            ],
            compiler_params=pltpu.CompilerParams(collective_id=0, has_side_effects=True, vmem_limit_bytes=56*1024*1024),
        )(lr_scale.reshape(epochs_t), rate_loc, mask_loc, user_loc, item_loc)
        return pl.pallas_call(
            write_out,
            out_shape=(jax.ShapeDtypeStruct(user_loc.shape, jnp.float32), jax.ShapeDtypeStruct(item_loc.shape, jnp.float32)),
            in_specs=[vmem, vmem],
            out_specs=(hbm, hbm),
            scratch_shapes=[pltpu.SemaphoreType.DMA((2, PARTS))],
            compiler_params=pltpu.CompilerParams(vmem_limit_bytes=1024 * 1024),
        )(users, items)

    spec_cols = P(None, ("rep", "blk"))
    spec_rows = P(("rep", "blk"), None)
    return jax.shard_map(local_run, mesh=mesh, in_specs=(spec_cols, spec_cols, spec_rows, spec_rows, P(None, None)),
                         out_specs=(spec_rows, spec_rows), check_vma=False)
```

```python
import functools
import math

import jax
import jax.numpy as jnp
from jax import lax
from jax.experimental import pallas as pl
from jax.experimental.pallas import tpu as pltpu
from jax.sharding import PartitionSpec as P

LAMBDA = 0.05
MESH = pl.DeviceIdType.MESH
CHUNK = 128
TILE = 1024
STRIP = 128
STAGES = 3


def run_kernel(group, epochs_t, base_eta, lr_hbm, r_hbm, m_hbm, u_hbm, v_hbm, uo_hbm, vo_hbm,
               lr, rate, mask, v, vb, gv, err, inb, outb, load_sem, r_sem, m_sem, send_sem, recv_sem, home_sem, lr_sem, credit):
    rep, me = lax.axis_index("rep"), lax.axis_index("blk")
    left, right = lax.rem(me + group - 1, group), lax.rem(me + 1, group)
    chunks = inb.shape[1]
    items = v.shape[0]
    loads = group * chunks

    def row_block(g):
        return lax.rem(me + g // chunks, group) * chunks + lax.rem(g, chunks)

    def rate_load(g):
        where = row_block(g)
        return pltpu.make_async_copy(r_hbm.at[pl.ds(pl.multiple_of(where * CHUNK, CHUNK), CHUNK)], rate.at[where], r_sem.at[lax.rem(g, STAGES)])

    def mask_load(g):
        where = row_block(g)
        slot = lax.rem(g, STAGES)
        return pltpu.make_async_copy(m_hbm.at[pl.ds(pl.multiple_of(where * CHUNK, CHUNK), CHUNK)], mask.at[slot], m_sem.at[slot])

    def send(t, c):
        slot = lax.rem(t, 2)
        return pltpu.make_async_remote_copy(
            src_ref=outb.at[slot, c], dst_ref=inb.at[1 - slot, c], send_sem=send_sem.at[slot, c],
            recv_sem=recv_sem.at[1 - slot, c], device_id=(rep, left), device_id_type=MESH)

    def send_home(t, c):
        slot = lax.rem(t, 2)
        return pltpu.make_async_remote_copy(
            src_ref=outb.at[slot, c], dst_ref=uo_hbm.at[pl.ds(pl.multiple_of(c * CHUNK, CHUNK), CHUNK)], send_sem=send_sem.at[slot, c],
            recv_sem=home_sem.at[c], device_id=(rep, left), device_id_type=MESH)

    def user_load(c):
        return pltpu.make_async_copy(u_hbm.at[pl.ds(c * CHUNK, CHUNK)], inb.at[0, c], recv_sem.at[0, c])

    def v_load(n):
        cols = pl.ds(n * TILE, TILE)
        return pltpu.make_async_copy(v_hbm.at[cols], v.at[cols], load_sem.at[n])

    tiles = items // TILE
    for n in range(tiles):
        v_load(n).start()
    user_load(0).start()
    rate_load(0).start()
    mask_load(0).start()
    rate_load(1).start()
    mask_load(1).start()
    lr_load = pltpu.make_async_copy(lr_hbm, lr, lr_sem)
    lr_load.start()

    barrier = pltpu.get_barrier_semaphore()
    for neighbour in (left, right):
        pl.semaphore_signal(barrier, inc=1, device_id=(rep, neighbour), device_id_type=MESH)

    def clear(n, carry):
        gv[pl.ds(pl.multiple_of(n * STRIP, STRIP), STRIP), :] = jnp.zeros((STRIP, gv.shape[1]), jnp.float32)
        return carry

    def convert(n, carry):
        cols = pl.ds(pl.multiple_of(n * STRIP, STRIP), STRIP)
        vb[cols, :] = v[cols, :].astype(jnp.bfloat16)
        return carry

    lax.fori_loop(0, items // STRIP, clear, 0)
    for n in range(tiles):
        v_load(n).wait()
        lax.fori_loop(n * TILE // STRIP, (n + 1) * TILE // STRIP, convert, 0)
    lr_load.wait()
    pl.semaphore_wait(barrier, 2)
    for c in range(1, chunks):
        user_load(c).start()

    def chunk_step(t, c, step_size, first):
        slot = lax.rem(t, 2)
        if first:
            g = t * chunks + c

            @pl.when(g + 2 < loads)
            def _():
                rate_load(g + 2).start()
                mask_load(g + 2).start()

            rate_load(g).wait()
            mask_load(g).wait()

        @pl.when(t == 0)
        def _():
            pltpu.make_async_copy(u_hbm.at[pl.ds(0, CHUNK)], inb.at[0, c], recv_sem.at[0, c]).wait()

        @pl.when(t > 0)
        def _():
            send(t - 1, c).wait_recv()

        @pl.when(t >= 2)
        def _():
            send(t, c).wait_send()

        where = lax.rem(me + t, group) * chunks + c
        users_bf = inb[slot, c].astype(jnp.bfloat16)
        for n in range(items // TILE):
            cols = pl.ds(n * TILE, TILE)
            approx = lax.dot_general(users_bf, vb[cols, :], (((1,), (1,)), ((), ())), preferred_element_type=jnp.float32)
            rates = rate[where, :, cols]
            if first:
                seen = mask[lax.rem(t * chunks + c, STAGES), :, cols] != 0
                rate[where, :, cols] = jnp.where(seen, rates, jnp.inf)
            else:
                seen = rates < jnp.inf
            err[:, cols] = jnp.where(seen, approx - rates, 0.0).astype(jnp.bfloat16)
        grad_u = jnp.dot(err[...], vb[...], preferred_element_type=jnp.float32)
        users = inb[slot, c]
        outb[slot, c] = users - step_size * (grad_u + LAMBDA * users)

        for n in range(items // TILE):
            cols = pl.ds(n * TILE, TILE)
            gv[cols, :] += lax.dot_general(err[:, cols], users_bf, (((0,), (0,)), ((), ())), preferred_element_type=jnp.float32)

        @pl.when(t < epochs_t - 2)
        def _():
            pl.semaphore_signal(credit, inc=1, device_id=(rep, right), device_id_type=MESH)

        @pl.when((t > 0) & (t < epochs_t - 1))
        def _():
            pl.semaphore_wait(credit, 1)

        @pl.when(t < epochs_t - 1)
        def _():
            send(t, c).start()

        @pl.when(t == epochs_t - 1)
        def _():
            send_home(t, c).start()

    def sub_epoch(first, t, carry):
        step_size = base_eta * lr[t]

        def body(c, inner):
            chunk_step(t, c, step_size, first)
            return inner

        lax.fori_loop(0, chunks, body, 0)

        def update(n, inner):
            cols = pl.ds(pl.multiple_of(n * STRIP, STRIP), STRIP)
            old = v[cols, :]
            new = old - step_size * (gv[cols, :] + LAMBDA * old)
            v[cols, :] = new
            vb[cols, :] = new.astype(jnp.bfloat16)
            gv[cols, :] = jnp.zeros((STRIP, v.shape[1]), jnp.float32)
            return inner

        lax.fori_loop(0, items // STRIP, update, 0)
        return carry

    lax.fori_loop(0, group, functools.partial(sub_epoch, True), 0)
    lax.fori_loop(group, epochs_t, functools.partial(sub_epoch, False), 0)

    vo_hbm[...] = v[...]
    for c in range(chunks):
        send(epochs_t - 2, c).wait_send()
        send_home(epochs_t - 1, c).wait_send()
        send_home(epochs_t - 1, c).wait_recv()


PARTS = 1


def write_out(u_vmem, v_vmem, uo_hbm, vo_hbm, sem):
    copies = []
    for k, (src, dst) in enumerate(((v_vmem, vo_hbm), (u_vmem, uo_hbm))):
        rows = src.shape[0] // PARTS
        for p in range(PARTS):
            part = pl.ds(p * rows, rows)
            copies.append(pltpu.make_async_copy(src.at[part], dst.at[part], sem.at[k, p]))
    for copy in copies:
        copy.start()
    for copy in copies:
        copy.wait()


def solution(mesh):
    group = mesh.shape["blk"]

    def local_run(rate_loc, mask_loc, user_loc, item_loc, lr_scale):
        block_rows, rank = user_loc.shape
        cols = item_loc.shape[0]
        epochs_t = lr_scale.shape[0]
        chunks = block_rows // CHUNK
        base_eta = math.sqrt(rank) / (4.0 * (cols + 2 * rank))
        vmem = pl.BlockSpec(memory_space=pltpu.VMEM)
        hbm = pl.BlockSpec(memory_space=pl.ANY)
        users, items = pl.pallas_call(
            functools.partial(run_kernel, group, epochs_t, base_eta),
            out_shape=(pltpu.VMEM(user_loc.shape, jnp.float32), pltpu.VMEM(item_loc.shape, jnp.float32)),
            in_specs=[hbm, hbm, hbm, hbm, hbm],
            out_specs=(vmem, vmem),
            scratch_shapes=[
                pltpu.SMEM((epochs_t,), jnp.float32),
                pltpu.VMEM((group * chunks, CHUNK, cols), jnp.float32),
                pltpu.VMEM((STAGES, CHUNK, cols), jnp.int32),
                pltpu.VMEM((cols, rank), jnp.float32),
                pltpu.VMEM((cols, rank), jnp.bfloat16),
                pltpu.VMEM((cols, rank), jnp.float32),
                pltpu.VMEM((CHUNK, cols), jnp.bfloat16),
                pltpu.VMEM((2, chunks, CHUNK, rank), jnp.float32),
                pltpu.VMEM((2, chunks, CHUNK, rank), jnp.float32),
                pltpu.SemaphoreType.DMA((cols // TILE,)),
                pltpu.SemaphoreType.DMA((STAGES,)),
                pltpu.SemaphoreType.DMA((STAGES,)),
                pltpu.SemaphoreType.DMA((2, chunks)),
                pltpu.SemaphoreType.DMA((2, chunks)),
                pltpu.SemaphoreType.DMA((chunks,)),
                pltpu.SemaphoreType.DMA,
                pltpu.SemaphoreType.REGULAR,
            ],
            compiler_params=pltpu.CompilerParams(collective_id=0, has_side_effects=True, vmem_limit_bytes=56*1024*1024),
        )(lr_scale.reshape(epochs_t), rate_loc, mask_loc, user_loc, item_loc)
        return pl.pallas_call(
            write_out,
            out_shape=(jax.ShapeDtypeStruct(user_loc.shape, jnp.float32), jax.ShapeDtypeStruct(item_loc.shape, jnp.float32)),
            in_specs=[vmem, vmem],
            out_specs=(hbm, hbm),
            scratch_shapes=[pltpu.SemaphoreType.DMA((2, PARTS))],
            compiler_params=pltpu.CompilerParams(vmem_limit_bytes=1024 * 1024),
        )(users, items)

    spec_cols = P(None, ("rep", "blk"))
    spec_rows = P(("rep", "blk"), None)
    return jax.shard_map(local_run, mesh=mesh, in_specs=(spec_cols, spec_cols, spec_rows, spec_rows, P(None, None)),
                         out_specs=(spec_rows, spec_rows), check_vma=False)
```

```python
import functools
import math

import jax
import jax.numpy as jnp
from jax import lax
from jax.experimental import pallas as pl
from jax.experimental.pallas import tpu as pltpu
from jax.sharding import PartitionSpec as P

LAMBDA = 0.05
MESH = pl.DeviceIdType.MESH
CHUNK = 128
TILE = 1024
STRIP = 128
STAGES = 3


def run_kernel(group, epochs_t, base_eta, lr_hbm, r_hbm, m_hbm, u_hbm, v_hbm, uo_hbm, vo_hbm,
               lr, rate, mask, v, vb, gv, err, inb, outb, load_sem, r_sem, m_sem, send_sem, recv_sem, home_sem, lr_sem, credit):
    rep, me = lax.axis_index("rep"), lax.axis_index("blk")
    left, right = lax.rem(me + group - 1, group), lax.rem(me + 1, group)
    chunks = inb.shape[1]
    items = v.shape[0]
    loads = group * chunks

    def row_block(g):
        return lax.rem(me + g // chunks, group) * chunks + lax.rem(g, chunks)

    def rate_load(g):
        where = row_block(g)
        return pltpu.make_async_copy(r_hbm.at[pl.ds(pl.multiple_of(where * CHUNK, CHUNK), CHUNK)], rate.at[where], r_sem.at[lax.rem(g, STAGES)])

    def mask_load(g):
        where = row_block(g)
        slot = lax.rem(g, STAGES)
        return pltpu.make_async_copy(m_hbm.at[pl.ds(pl.multiple_of(where * CHUNK, CHUNK), CHUNK)], mask.at[slot], m_sem.at[slot])

    def send(t, c):
        slot = lax.rem(t, 2)
        return pltpu.make_async_remote_copy(
            src_ref=outb.at[slot, c], dst_ref=inb.at[1 - slot, c], send_sem=send_sem.at[slot, c],
            recv_sem=recv_sem.at[1 - slot, c], device_id=(rep, left), device_id_type=MESH)

    def send_home(t, c):
        slot = lax.rem(t, 2)
        return pltpu.make_async_remote_copy(
            src_ref=outb.at[slot, c], dst_ref=uo_hbm.at[pl.ds(pl.multiple_of(c * CHUNK, CHUNK), CHUNK)], send_sem=send_sem.at[slot, c],
            recv_sem=home_sem.at[c], device_id=(rep, left), device_id_type=MESH)

    def user_load(c):
        return pltpu.make_async_copy(u_hbm.at[pl.ds(c * CHUNK, CHUNK)], inb.at[0, c], recv_sem.at[0, c])

    def v_load(n):
        cols = pl.ds(n * TILE, TILE)
        return pltpu.make_async_copy(v_hbm.at[cols], v.at[cols], load_sem.at[n])

    tiles = items // TILE
    for n in range(tiles):
        v_load(n).start()
    user_load(0).start()
    rate_load(0).start()
    mask_load(0).start()
    rate_load(1).start()
    mask_load(1).start()
    lr_load = pltpu.make_async_copy(lr_hbm, lr, lr_sem)
    lr_load.start()

    barrier = pltpu.get_barrier_semaphore()
    for neighbour in (left, right):
        pl.semaphore_signal(barrier, inc=1, device_id=(rep, neighbour), device_id_type=MESH)

    def clear(n, carry):
        gv[pl.ds(pl.multiple_of(n * STRIP, STRIP), STRIP), :] = jnp.zeros((STRIP, gv.shape[1]), jnp.float32)
        return carry

    def convert(n, carry):
        cols = pl.ds(pl.multiple_of(n * STRIP, STRIP), STRIP)
        vb[cols, :] = v[cols, :].astype(jnp.bfloat16)
        return carry

    lax.fori_loop(0, items // STRIP, clear, 0)
    for n in range(tiles):
        v_load(n).wait()
        lax.fori_loop(n * TILE // STRIP, (n + 1) * TILE // STRIP, convert, 0)
    for c in range(1, chunks):
        user_load(c).start()
    lr_load.wait()
    pl.semaphore_wait(barrier, 2)

    def chunk_step(t, c, step_size, first):
        slot = lax.rem(t, 2)
        if first:
            g = t * chunks + c

            @pl.when(g + 2 < loads)
            def _():
                rate_load(g + 2).start()
                mask_load(g + 2).start()

            rate_load(g).wait()
            mask_load(g).wait()

        @pl.when(t == 0)
        def _():
            pltpu.make_async_copy(u_hbm.at[pl.ds(0, CHUNK)], inb.at[0, c], recv_sem.at[0, c]).wait()

        @pl.when(t > 0)
        def _():
            send(t - 1, c).wait_recv()

        @pl.when(t >= 2)
        def _():
            send(t, c).wait_send()

        where = lax.rem(me + t, group) * chunks + c
        users_bf = inb[slot, c].astype(jnp.bfloat16)
        for n in range(items // TILE):
            cols = pl.ds(n * TILE, TILE)
            approx = lax.dot_general(users_bf, vb[cols, :], (((1,), (1,)), ((), ())), preferred_element_type=jnp.float32)
            rates = rate[where, :, cols]
            if first:
                seen = mask[lax.rem(t * chunks + c, STAGES), :, cols] != 0
                rate[where, :, cols] = jnp.where(seen, rates, jnp.inf)
            else:
                seen = rates < jnp.inf
            err[:, cols] = jnp.where(seen, approx - rates, 0.0).astype(jnp.bfloat16)
        grad_u = jnp.dot(err[...], vb[...], preferred_element_type=jnp.float32)
        users = inb[slot, c]
        outb[slot, c] = users - step_size * (grad_u + LAMBDA * users)

        for n in range(items // TILE):
            cols = pl.ds(n * TILE, TILE)
            gv[cols, :] += lax.dot_general(err[:, cols], users_bf, (((0,), (0,)), ((), ())), preferred_element_type=jnp.float32)

        @pl.when(t < epochs_t - 2)
        def _():
            pl.semaphore_signal(credit, inc=1, device_id=(rep, right), device_id_type=MESH)

        @pl.when((t > 0) & (t < epochs_t - 1))
        def _():
            pl.semaphore_wait(credit, 1)

        @pl.when(t < epochs_t - 1)
        def _():
            send(t, c).start()

        @pl.when(t == epochs_t - 1)
        def _():
            send_home(t, c).start()

    def sub_epoch(first, t, carry):
        step_size = base_eta * lr[t]

        def body(c, inner):
            chunk_step(t, c, step_size, first)
            return inner

        lax.fori_loop(0, chunks, body, 0)

        def update(n, inner):
            cols = pl.ds(pl.multiple_of(n * STRIP, STRIP), STRIP)
            old = v[cols, :]
            new = old - step_size * (gv[cols, :] + LAMBDA * old)
            v[cols, :] = new
            vb[cols, :] = new.astype(jnp.bfloat16)
            gv[cols, :] = jnp.zeros((STRIP, v.shape[1]), jnp.float32)
            return inner

        lax.fori_loop(0, items // STRIP, update, 0)
        return carry

    lax.fori_loop(0, group, functools.partial(sub_epoch, True), 0)
    lax.fori_loop(group, epochs_t, functools.partial(sub_epoch, False), 0)

    vo_hbm[...] = v[...]
    for c in range(chunks):
        send(epochs_t - 2, c).wait_send()
        send_home(epochs_t - 1, c).wait_send()
        send_home(epochs_t - 1, c).wait_recv()


PARTS = 1


def write_out(u_vmem, v_vmem, uo_hbm, vo_hbm, sem):
    copies = []
    for k, (src, dst) in enumerate(((v_vmem, vo_hbm), (u_vmem, uo_hbm))):
        rows = src.shape[0] // PARTS
        for p in range(PARTS):
            part = pl.ds(p * rows, rows)
            copies.append(pltpu.make_async_copy(src.at[part], dst.at[part], sem.at[k, p]))
    for copy in copies:
        copy.start()
    for copy in copies:
        copy.wait()


def solution(mesh):
    group = mesh.shape["blk"]

    def local_run(rate_loc, mask_loc, user_loc, item_loc, lr_scale):
        block_rows, rank = user_loc.shape
        cols = item_loc.shape[0]
        epochs_t = lr_scale.shape[0]
        chunks = block_rows // CHUNK
        base_eta = math.sqrt(rank) / (4.0 * (cols + 2 * rank))
        vmem = pl.BlockSpec(memory_space=pltpu.VMEM)
        hbm = pl.BlockSpec(memory_space=pl.ANY)
        users, items = pl.pallas_call(
            functools.partial(run_kernel, group, epochs_t, base_eta),
            out_shape=(pltpu.VMEM(user_loc.shape, jnp.float32), pltpu.VMEM(item_loc.shape, jnp.float32)),
            in_specs=[hbm, hbm, hbm, hbm, hbm],
            out_specs=(vmem, vmem),
            scratch_shapes=[
                pltpu.SMEM((epochs_t,), jnp.float32),
                pltpu.VMEM((group * chunks, CHUNK, cols), jnp.float32),
                pltpu.VMEM((STAGES, CHUNK, cols), jnp.int32),
                pltpu.VMEM((cols, rank), jnp.float32),
                pltpu.VMEM((cols, rank), jnp.bfloat16),
                pltpu.VMEM((cols, rank), jnp.float32),
                pltpu.VMEM((CHUNK, cols), jnp.bfloat16),
                pltpu.VMEM((2, chunks, CHUNK, rank), jnp.float32),
                pltpu.VMEM((2, chunks, CHUNK, rank), jnp.float32),
                pltpu.SemaphoreType.DMA((cols // TILE,)),
                pltpu.SemaphoreType.DMA((STAGES,)),
                pltpu.SemaphoreType.DMA((STAGES,)),
                pltpu.SemaphoreType.DMA((2, chunks)),
                pltpu.SemaphoreType.DMA((2, chunks)),
                pltpu.SemaphoreType.DMA((chunks,)),
                pltpu.SemaphoreType.DMA,
                pltpu.SemaphoreType.REGULAR,
            ],
            compiler_params=pltpu.CompilerParams(collective_id=0, has_side_effects=True, vmem_limit_bytes=56*1024*1024),
        )(lr_scale.reshape(epochs_t), rate_loc, mask_loc, user_loc, item_loc)
        return pl.pallas_call(
            write_out,
            out_shape=(jax.ShapeDtypeStruct(user_loc.shape, jnp.float32), jax.ShapeDtypeStruct(item_loc.shape, jnp.float32)),
            in_specs=[vmem, vmem],
            out_specs=(hbm, hbm),
            scratch_shapes=[pltpu.SemaphoreType.DMA((2, PARTS))],
            compiler_params=pltpu.CompilerParams(vmem_limit_bytes=1024 * 1024),
        )(users, items)

    spec_cols = P(None, ("rep", "blk"))
    spec_rows = P(("rep", "blk"), None)
    return jax.shard_map(local_run, mesh=mesh, in_specs=(spec_cols, spec_cols, spec_rows, spec_rows, P(None, None)),
                         out_specs=(spec_rows, spec_rows), check_vma=False)
```
